32 devices in a mesh: seq: 16 (over z, y, x), tensor: 2 (over core).
Axes of the slice: x: 2, y: 2, z: 4, core: 2. Of those that a mesh axis runs over, the one named last changes fastest.
Arguments:
- hidden: bfloat16 [2, 4096, 8192], P(None, 'seq', 'tensor'), may hold values from -160 to 160
- norm_gain: bfloat16 [8192], P('tensor'), may hold values from 0.25 to 1.75
- value_weight: bfloat16 [8192], P('tensor'), may hold values from -0.0625 to 0.0625
- rewards: float32 [2, 4096], P(None, 'seq'), may hold values from -6 to 6
- done_flags: int32 [2, 4096], P(None, 'seq'), may hold values 0 or 1
- valid_mask: int32 [2, 4096], P('tensor', 'seq'), may hold values 0 or 1
- new_logprob: float32 [2, 4096], P('tensor', 'seq'), may hold values from -1 to 1
- old_logprob: float32 [2, 4096], P('tensor', 'seq'), may hold values from -1 to 1
- discount: float32 [2], replicated, may hold values from 0.9 to 1
- trace_decay: float32 [2], replicated, may hold values from 0.9 to 1
- bootstrap: float32 [2], replicated, may hold values from -5 to 5
Outputs:
- values: float32 [2, 4096], P('tensor', 'seq')
- white_adv: float32 [2, 4096], P('tensor', 'seq')
- token_loss: float32 [2, 4096], P('tensor', 'seq')
- policy_loss: float32 [], replicated
The draws below stay inside these ranges and needn't reach their ends.
All inputs are finite; a program needn't handle non-finite values. No bound on the sum of `done_flags` or of `valid_mask` on one device may be relied on, other than what follows from the above.
Results may differ from the reference program's by a relative error of at most 0.00035.
Values sent between devices are 32-bit elements; how exact they have to be, the bound alone decides.
A program may use at most 64 MiB of HBM per device.

```python
import math
from functools import partial
import jax
import jax.numpy as jnp
from jax import lax

H = 8192
LEN_DEV = 256
SEQS = 2
LENGTH = 4096


def draw_hidden(key, part):
    k_base, k_cols = jax.random.split(jax.random.fold_in(key, 11), 2)
    base = jax.random.truncated_normal(k_base, -4.0, 4.0, (SEQS, LENGTH, H), jnp.float32)
    columns = jnp.exp(jax.random.uniform(k_cols, (H,), jnp.float32) * math.log(10.0))
    drawn = base * columns
    return drawn.astype(jnp.bfloat16)


def draw_discount(key, part):
    k_main = jax.random.fold_in(key, 23)
    spread = jax.random.uniform(k_main, (SEQS,), jnp.float32, 0.1, 0.5)
    return 1.0 - spread / LENGTH


def draw_trace_decay(key, part):
    k_pick, k_slow, k_fast = jax.random.split(jax.random.fold_in(key, 37), 3)
    quick = jax.random.bernoulli(k_pick, 0.5, (SEQS,))
    slow_rate = 1.0 - jax.random.uniform(k_slow, (SEQS,), jnp.float32, 0.2, 1.0) / LENGTH
    fast_rate = 1.0 - jax.random.uniform(k_fast, (SEQS,), jnp.float32, 0.02, 0.033)
    return jnp.where(quick, fast_rate, slow_rate)


def touch_ends(entries, stream_key, low, largest):
    index_at = [jax.random.randint(jax.random.fold_in(stream_key, axis), (), 0, length) for axis, length in enumerate(entries.shape)]
    longest = entries.shape.index(max(entries.shape))
    beside = index_at[:longest] + [(index_at[longest] + 1) % entries.shape[longest]] + index_at[longest + 1:]
    return entries.at[tuple(index_at)].set(low).at[tuple(beside)].set(largest)


def block_scale(own_key, extent, shards, smallest, high):
    factor_of = 1.0
    for position, parts in shards:
        steps = jax.random.uniform(jax.random.fold_in(jax.random.fold_in(own_key, 6), position), (parts,), jnp.float32, smallest / len(shards), high / len(shards))
        factor_of = factor_of * jnp.repeat(jnp.exp(steps), extent[position] // parts).reshape((-1,) + (1,) * (len(extent) - 1 - position))
    return factor_of


def noise(key, dims, deviation, limit, shards=(), held_as=jnp.bfloat16):
    values = deviation * jax.random.normal(key, dims, jnp.float32)
    if shards:
        values = values * block_scale(key, dims, shards, -0.22, 0.18)
    return jnp.clip(values, -limit, limit).astype(held_as)


def setup_inputs(seed: int = 0) -> dict:
    seeds = jax.random.split(jax.random.key(seed), 12)
    return {
        "hidden": draw_hidden(jax.random.fold_in(seeds[11], 71), 0),
        "norm_gain": jnp.clip(1.0 + 0.15 * jax.random.normal(seeds[1], (H,), jnp.float32), 0.25, 1.75).astype(jnp.bfloat16),
        "value_weight": noise(seeds[2], (H,), H ** -0.5, 0.0625, ((0, 2),)),
        "rewards": noise(seeds[3], (SEQS, LENGTH), 1.0, 6.0, ((1, 16),), jnp.float32),
        "done_flags": touch_ends((jax.random.randint(seeds[4], (SEQS, LENGTH), 0, 128 * LEN_DEV) < 1).astype(jnp.int32), jax.random.fold_in(seeds[4], 1), 0, 1),
        "valid_mask": touch_ends((jax.random.randint(seeds[5], (SEQS, LENGTH), 0, 4) < 3).astype(jnp.int32), jax.random.fold_in(seeds[5], 1), 0, 1),
        "new_logprob": noise(seeds[6], (SEQS, LENGTH), 0.15, 1.0, ((0, 2), (1, 16)), jnp.float32),
        "old_logprob": noise(seeds[7], (SEQS, LENGTH), 0.15, 1.0, ((0, 2), (1, 16)), jnp.float32),
        "discount": draw_discount(jax.random.fold_in(seeds[11], 71), 0),
        "trace_decay": draw_trace_decay(jax.random.fold_in(seeds[11], 71), 0),
        "bootstrap": noise(seeds[10], (SEQS,), 1.0, 5.0, (), jnp.float32),
    }


EPS_NORM = 1e-06
EPS_WHITE = 1e-08
CLIP = 0.2

def head_block(scaled, block):
    wide = block.astype(jnp.float32)
    squares = lax.optimization_barrier(jnp.sum(wide * wide, axis=-1))
    products = jnp.dot(wide, scaled, precision=lax.Precision.HIGHEST)
    return products * lax.rsqrt(squares / H + EPS_NORM)

def backward_step(carry, inputs):
    delta_now, coef_now = inputs
    fresh = delta_now + coef_now * carry
    return (fresh, fresh)

def reference(hidden, norm_gain, value_weight, rewards, done_flags, valid_mask, new_logprob, old_logprob, discount, trace_decay, bootstrap):
    scaled = norm_gain.astype(jnp.float32) * value_weight.astype(jnp.float32)
    blocks = hidden.reshape(SEQS * LENGTH // LEN_DEV, LEN_DEV, H)
    values = lax.map(partial(head_block, scaled), blocks).reshape(SEQS, LENGTH)
    alive = 1.0 - done_flags.astype(jnp.float32)
    following = jnp.concatenate([values[:, 1:], bootstrap[:, None]], axis=1)
    delta = rewards + discount[:, None] * alive * following - values
    decay = discount * trace_decay
    coefs = decay[:, None] * alive
    start = jnp.zeros((SEQS,), jnp.float32)
    _, stacked = lax.scan(backward_step, start, (delta.T, coefs.T), reverse=True)
    advantages = stacked.T
    weight = valid_mask.astype(jnp.float32)
    count = jnp.sum(weight)
    mean = jnp.sum(weight * advantages) / count
    variance = jnp.sum(weight * (advantages - mean) ** 2) / count
    white_adv = (advantages - mean) * lax.rsqrt(variance + EPS_WHITE)
    ratio = jnp.exp(new_logprob - old_logprob)
    surrogate = jnp.minimum(ratio * white_adv, jnp.clip(ratio, 1.0 - CLIP, 1.0 + CLIP) * white_adv)
    token_loss = -weight * surrogate
    policy_loss = jnp.sum(token_loss) / count
    return (values, white_adv, token_loss, policy_loss)
```

```python
import functools

import jax
import jax.numpy as jnp
from jax import lax
from jax.experimental import pallas as pl
from jax.experimental.pallas import tpu as pltpu
from jax.sharding import PartitionSpec as P

EPS_NORM = 1e-06
EPS_WHITE = 1e-08
CLIP = 0.2
HIGHEST = lax.Precision.HIGHEST
LANES = 128
BLOCK = 32


def lane_sums(parts):
    ones = jnp.ones((8, LANES), jnp.float32)
    return lax.dot_general(
        ones, parts, (((1,), (1,)), ((), ())), precision=HIGHEST, preferred_element_type=jnp.float32
    )


def kernel(
    seq_count,
    tensor_count,
    width,
    chunk,
    hidden_hbm,
    gain_hbm,
    weight_hbm,
    rewards_hbm,
    flags_hbm,
    mask_hbm,
    new_hbm,
    old_hbm,
    discount_hbm,
    trace_hbm,
    boot_hbm,
    values_ref,
    white_ref,
    token_ref,
    loss_ref,
    hid,
    gain,
    wgt,
    rew,
    flg,
    msk,
    newp,
    oldp,
    disc,
    trc,
    boot,
    scaled,
    parts,
    part_send,
    part_recv,
    early,
    late,
    carry,
    hid_sem,
    in_sem,
    part_send_sem,
    part_recv_sem,
    early_send_sem,
    early_recv_sem,
    late_send_sem,
    late_recv_sem,
):
    seqs_all, length, local_width = hid.shape
    own_rows = seqs_all // tensor_count
    devices = seq_count * tensor_count
    chunks = length // chunk
    me_seq = lax.axis_index("seq")
    me_ten = lax.axis_index("tensor")
    first_row = me_ten * own_rows
    my_slot = me_ten * seq_count + me_seq

    small = [
        (gain_hbm, gain),
        (weight_hbm, wgt),
        (rewards_hbm, rew),
        (flags_hbm, flg),
        (mask_hbm, msk),
        (new_hbm, newp),
        (old_hbm, oldp),
        (discount_hbm, disc),
        (trace_hbm, trc),
        (boot_hbm, boot),
    ]
    small_copies = [
        pltpu.make_async_copy(src, dst, in_sem.at[i]) for i, (src, dst) in enumerate(small)
    ]
    for copy in small_copies:
        copy.start()

    def hid_copy(i, c):
        row = lax.rem(first_row + own_rows + i, seqs_all)
        rows = pl.ds(pl.multiple_of(c * chunk, chunk), chunk)
        return pltpu.make_async_copy(
            hidden_hbm.at[row, rows, :], hid.at[i, rows, :], hid_sem.at[i * chunks + c]
        )

    for i in range(seqs_all):
        for c in range(chunks):
            hid_copy(i, c).start()

    barrier = pltpu.get_barrier_semaphore()

    def peer(k):
        slot = lax.rem(my_slot + k, devices)
        return (lax.rem(slot, seq_count), lax.div(slot, seq_count))

    def greet(k, _):
        pl.semaphore_signal(
            barrier, inc=1, device_id=peer(k), device_id_type=pl.DeviceIdType.MESH
        )
        return 0

    lax.fori_loop(1, devices, greet, 0)

    for copy in small_copies:
        copy.wait()

    for j in range(local_width // LANES):
        cols = pl.ds(j * LANES, LANES)
        row = gain[0:1, cols].astype(jnp.float32) * wgt[0:1, cols].astype(jnp.float32)
        scaled[:, cols] = jnp.broadcast_to(row, (8, LANES))

    lane = lax.broadcasted_iota(jnp.int32, (8, length), 1)
    steps = []
    step = 1
    while step < length:
        steps.append(step)
        step *= 2
    ahead = lambda x, d: pltpu.roll(x, length - d, 1)
    rows_info = []
    for r in range(own_rows):
        discount = jnp.full((8, length), disc[first_row + r], jnp.float32)
        trace = jnp.full((8, length), trc[first_row + r], jnp.float32)
        flags = jnp.broadcast_to(flg[pl.ds(first_row + r, 1), :], (8, length))
        alive = 1.0 - flags.astype(jnp.float32)
        link = discount * trace * alive
        level = jnp.where(lane < length - 1, link, 0.0)
        coef = jnp.where(lane < length - 1, link, discount * alive)
        levels = []
        for d in steps:
            levels.append(level)
            level = level * ahead(level, d)
            coef = coef * jnp.where(lane < length - d, ahead(coef, d), 1.0)
        ratio = jnp.exp(newp[r : r + 1, :] - oldp[r : r + 1, :])
        weight = msk[r : r + 1, :].astype(jnp.float32)
        reward = jnp.broadcast_to(rew[pl.ds(first_row + r, 1), :], (8, length))
        following = jnp.where(lane < length - 1, discount * alive, 0.0)
        rows_info.append((trace, levels, coef, ratio, weight, reward, following))
        early[my_slot, r : r + 1, 0:length] = ratio
        early[my_slot, r : r + 1, length : 2 * length] = weight
        early[my_slot, r : r + 1, 2 * length : 3 * length] = coef[0:1, :]
        early[my_slot, r : r + 1, 3 * length : 3 * length + LANES] = jnp.broadcast_to(
            trace[0:1, 0:1] * coef[0:1, 0:1], (1, LANES)
        )

    def row_sums(i):
        def do_chunk(c, _):
            hid_copy(i, c).wait()
            for b in range(chunk // BLOCK):
                rows = pl.ds(pl.multiple_of(c * chunk + b * BLOCK, BLOCK), BLOCK)
                squares = jnp.zeros((BLOCK // 8, 8, LANES), jnp.float32)
                products = jnp.zeros((BLOCK // 8, 8, LANES), jnp.float32)
                for j in range(local_width // LANES):
                    cols = pl.ds(j * LANES, LANES)
                    x = hid[i, rows, cols].astype(jnp.float32).reshape(BLOCK // 8, 8, LANES)
                    squares = squares + x * x
                    products = products + x * scaled[:, cols][None]
                parts[0, rows, :] = squares.reshape(BLOCK, LANES)
                parts[1, rows, :] = products.reshape(BLOCK, LANES)
            return 0

        lax.fori_loop(0, chunks, do_chunk, 0)
        return lane_sums(parts[0]), lane_sums(parts[1])

    for k in range(1, tensor_count):
        for r in range(own_rows):
            squares, products = row_sums((k - 1) * own_rows + r)
            part_send[k - 1, 2 * r : 2 * r + 1, :] = squares[0:1, :]
            part_send[k - 1, 2 * r + 1 : 2 * r + 2, :] = products[0:1, :]

    pl.semaphore_wait(barrier, devices - 1)

    part_copies = []
    for k in range(1, tensor_count):
        copy = pltpu.make_async_remote_copy(
            src_ref=part_send.at[k - 1],
            dst_ref=part_recv.at[k - 1],
            send_sem=part_send_sem.at[k - 1],
            recv_sem=part_recv_sem.at[k - 1],
            device_id=(me_seq, lax.rem(me_ten + k, tensor_count)),
            device_id_type=pl.DeviceIdType.MESH,
        )
        copy.start()
        part_copies.append(copy)

    def send_all(buffer, send_sem, recv_sem):
        def send(k, _):
            pltpu.make_async_remote_copy(
                src_ref=buffer.at[my_slot],
                dst_ref=buffer.at[my_slot],
                send_sem=send_sem,
                recv_sem=recv_sem,
                device_id=peer(k),
                device_id_type=pl.DeviceIdType.MESH,
            ).start()
            return 0

        lax.fori_loop(1, devices, send, 0)

    def all_blocks(buffer, sem):
        view = buffer.at[pl.ds(0, devices - 1)]
        return pltpu.make_async_copy(view, view, sem)

    send_all(early, early_send_sem, early_recv_sem)

    own = [row_sums((tensor_count - 1) * own_rows + r) for r in range(own_rows)]
    for copy in part_copies:
        copy.wait()

    for r in range(own_rows):
        trace, levels, coef, ratio, weight, reward, following = rows_info[r]
        squares, products = own[r]
        for k in range(1, tensor_count):
            squares = squares + part_recv[k - 1, 2 * r : 2 * r + 1, :]
            products = products + part_recv[k - 1, 2 * r + 1 : 2 * r + 2, :]
        values = products * lax.rsqrt(squares / width + EPS_NORM)
        values_ref[r : r + 1, :] = values[0:1, :]
        adv = reward + following * ahead(values, 1) - values
        for d, level in zip(steps, levels):
            adv = adv + level * ahead(adv, d)
        late[my_slot, r : r + 1, 0:length] = adv[0:1, :]
        late[my_slot, r : r + 1, length : length + LANES] = jnp.broadcast_to(
            values[0:1, 0:1] + trace[0:1, 0:1] * adv[0:1, 0:1], (1, LANES)
        )

    send_all(late, late_send_sem, late_recv_sem)

    all_blocks(early, early_recv_sem).wait()
    count = jnp.zeros((seq_count, length), jnp.float32)
    for t in range(tensor_count):
        for r in range(own_rows):
            count = count + early[pl.ds(t * seq_count, seq_count), r, length : 2 * length]
    total = lambda x: jnp.sum(jnp.sum(x, axis=0, keepdims=True), axis=1, keepdims=True)
    count = total(count)
    all_blocks(late, late_recv_sem).wait()

    advs = []
    for t in range(tensor_count):
        for r in range(own_rows):
            entering = jnp.full((1, LANES), boot[t * own_rows + r], jnp.float32)
            for n in range(seq_count - 1, -1, -1):
                slot = t * seq_count + n
                carry[slot, r : r + 1, :] = entering
                if n:
                    offset = late[slot, r : r + 1, length : length + LANES]
                    slope = early[slot, r : r + 1, 3 * length : 3 * length + LANES]
                    entering = offset + slope * entering
    sums = jnp.zeros((seq_count, length), jnp.float32)
    for t in range(tensor_count):
        for r in range(own_rows):
            slots = pl.ds(t * seq_count, seq_count)
            entering = jnp.concatenate([carry[slots, r, :]] * (length // LANES), axis=1)
            adv = late[slots, r, 0:length] + early[slots, r, 2 * length : 3 * length] * entering
            advs.append(adv)
            sums = sums + early[slots, r, length : 2 * length] * adv
    mean = total(sums) / count
    sums = jnp.zeros((seq_count, length), jnp.float32)
    for t in range(tensor_count):
        for r in range(own_rows):
            slots = pl.ds(t * seq_count, seq_count)
            centred = advs[t * own_rows + r] - mean
            advs[t * own_rows + r] = centred
            sums = sums + early[slots, r, length : 2 * length] * centred * centred
    scale = lax.rsqrt(total(sums) / count + EPS_WHITE)

    def token_loss(ratio, weight, white):
        clipped = jnp.clip(ratio, 1.0 - CLIP, 1.0 + CLIP)
        return -weight * jnp.minimum(ratio * white, clipped * white)

    for r in range(own_rows):
        _, _, coef, ratio, weight, _, _ = rows_info[r]
        entering = carry[my_slot, r : r + 1, :]
        entering = jnp.concatenate([entering] * (length // LANES), axis=1)
        adv = late[my_slot, r : r + 1, 0:length] + coef[0:1, :] * entering
        white = (adv - mean) * scale
        white_ref[r : r + 1, :] = white
        token_ref[r : r + 1, :] = token_loss(ratio, weight, white)

    sums = jnp.zeros((seq_count, length), jnp.float32)
    for t in range(tensor_count):
        for r in range(own_rows):
            slots = pl.ds(t * seq_count, seq_count)
            sums = sums + token_loss(
                early[slots, r, 0:length],
                early[slots, r, length : 2 * length],
                advs[t * own_rows + r] * scale,
            )
    loss_ref[...] = total(sums) / count

    all_blocks(early, early_send_sem).wait()
    all_blocks(late, late_send_sem).wait()


def shards(seq_count, tensor_count, hidden, norm_gain, value_weight, *rest):
    seqs_all, length, local_width = hidden.shape
    own_rows = seqs_all // tensor_count
    devices = seq_count * tensor_count
    chunk = min(length, 64)
    f32 = jnp.float32
    row = jax.ShapeDtypeStruct((own_rows, length), f32)
    dma = pltpu.SemaphoreType.DMA
    outs = pl.pallas_call(
        functools.partial(kernel, seq_count, tensor_count, local_width * tensor_count, chunk),
        out_shape=[row, row, row, jax.ShapeDtypeStruct((1, 1), f32)],
        in_specs=[pl.BlockSpec(memory_space=pl.ANY)] * 11,
        out_specs=[pl.BlockSpec(memory_space=pltpu.VMEM)] * 4,
        scratch_shapes=[
            pltpu.VMEM((seqs_all, length, local_width), jnp.bfloat16),
            pltpu.VMEM((1, local_width), jnp.bfloat16),
            pltpu.VMEM((1, local_width), jnp.bfloat16),
            pltpu.VMEM((seqs_all, length), f32),
            pltpu.VMEM((seqs_all, length), jnp.int32),
            pltpu.VMEM((own_rows, length), jnp.int32),
            pltpu.VMEM((own_rows, length), f32),
            pltpu.VMEM((own_rows, length), f32),
            pltpu.SMEM((seqs_all,), f32),
            pltpu.SMEM((seqs_all,), f32),
            pltpu.SMEM((seqs_all,), f32),
            pltpu.VMEM((8, local_width), f32),
            pltpu.VMEM((2, length, LANES), f32),
            pltpu.VMEM((max(tensor_count - 1, 1), 2 * own_rows, length), f32),
            pltpu.VMEM((max(tensor_count - 1, 1), 2 * own_rows, length), f32),
            pltpu.VMEM((devices, own_rows, 3 * length + LANES), f32),
            pltpu.VMEM((devices, own_rows, length + LANES), f32),
            pltpu.VMEM((devices, own_rows, LANES), f32),
            dma((seqs_all * (length // chunk),)),
            dma((10,)),
            dma((max(tensor_count - 1, 1),)),
            dma((max(tensor_count - 1, 1),)),
            dma,
            dma,
            dma,
            dma,
        ],
        compiler_params=pltpu.CompilerParams(collective_id=0, has_side_effects=True),
    )(hidden, norm_gain.reshape(1, -1), value_weight.reshape(1, -1), *rest)
    return (outs[0], outs[1], outs[2], outs[3].reshape(()))


def solution(mesh):
    in_specs = (
        P(None, "seq", "tensor"),
        P("tensor"),
        P("tensor"),
        P(None, "seq"),
        P(None, "seq"),
        P("tensor", "seq"),
        P("tensor", "seq"),
        P("tensor", "seq"),
        P(),
        P(),
        P(),
    )
    out_specs = (P("tensor", "seq"), P("tensor", "seq"), P("tensor", "seq"), P())
    body = functools.partial(shards, mesh.shape["seq"], mesh.shape["tensor"])
    return jax.shard_map(body, mesh=mesh, in_specs=in_specs, out_specs=out_specs, check_vma=False)
```

```python
import functools

import jax
import jax.numpy as jnp
from jax import lax
from jax.experimental import pallas as pl
from jax.experimental.pallas import tpu as pltpu
from jax.sharding import PartitionSpec as P

EPS_NORM = 1e-06
EPS_WHITE = 1e-08
CLIP = 0.2
HIGHEST = lax.Precision.HIGHEST
LANES = 128
BLOCK = 32


def lane_sums(parts):
    ones = jnp.ones((8, LANES), jnp.float32)
    return lax.dot_general(
        ones, parts, (((1,), (1,)), ((), ())), precision=HIGHEST, preferred_element_type=jnp.float32
    )


def kernel(
    seq_count,
    tensor_count,
    width,
    chunk,
    hidden_hbm,
    gain_hbm,
    weight_hbm,
    rewards_hbm,
    flags_hbm,
    mask_hbm,
    new_hbm,
    old_hbm,
    discount_hbm,
    trace_hbm,
    boot_hbm,
    values_ref,
    white_ref,
    token_ref,
    loss_ref,
    hid,
    gain,
    wgt,
    rew,
    flg,
    msk,
    newp,
    oldp,
    disc,
    trc,
    boot,
    scaled,
    parts,
    part_send,
    part_recv,
    early,
    late,
    carry,
    hid_sem,
    in_sem,
    part_send_sem,
    part_recv_sem,
    early_send_sem,
    early_recv_sem,
    late_send_sem,
    late_recv_sem,
):
    seqs_all, length, local_width = hid.shape
    own_rows = seqs_all // tensor_count
    devices = seq_count * tensor_count
    chunks = length // chunk
    me_seq = lax.axis_index("seq")
    me_ten = lax.axis_index("tensor")
    first_row = me_ten * own_rows
    my_slot = me_ten * seq_count + me_seq

    small = [
        (gain_hbm, gain),
        (weight_hbm, wgt),
        (rewards_hbm, rew),
        (flags_hbm, flg),
        (mask_hbm, msk),
        (new_hbm, newp),
        (old_hbm, oldp),
        (discount_hbm, disc),
        (trace_hbm, trc),
        (boot_hbm, boot),
    ]
    small_copies = [
        pltpu.make_async_copy(src, dst, in_sem.at[i]) for i, (src, dst) in enumerate(small)
    ]
    for copy in small_copies:
        copy.start()

    def hid_copy(i, c):
        row = lax.rem(first_row + own_rows + i, seqs_all)
        rows = pl.ds(pl.multiple_of(c * chunk, chunk), chunk)
        return pltpu.make_async_copy(
            hidden_hbm.at[row, rows, :], hid.at[i, rows, :], hid_sem.at[i * chunks + c]
        )

    for i in range(seqs_all):
        for c in range(chunks):
            hid_copy(i, c).start()

    barrier = pltpu.get_barrier_semaphore()

    def peer(k):
        slot = lax.rem(my_slot + k, devices)
        return (lax.rem(slot, seq_count), lax.div(slot, seq_count))

    def greet(k, _):
        pl.semaphore_signal(
            barrier, inc=1, device_id=peer(k), device_id_type=pl.DeviceIdType.MESH
        )
        return 0

    lax.fori_loop(1, devices, greet, 0)

    for copy in small_copies:
        copy.wait()

    for j in range(local_width // LANES):
        cols = pl.ds(j * LANES, LANES)
        row = gain[cols].astype(jnp.float32) * wgt[cols].astype(jnp.float32)
        scaled[:, cols] = jnp.broadcast_to(row.reshape(1, LANES), (8, LANES))

    lane = lax.broadcasted_iota(jnp.int32, (8, length), 1)
    steps = []
    step = 1
    while step < length:
        steps.append(step)
        step *= 2
    ahead = lambda x, d: pltpu.roll(x, length - d, 1)
    rows_info = []
    for r in range(own_rows):
        discount = jnp.full((8, length), disc[first_row + r], jnp.float32)
        trace = jnp.full((8, length), trc[first_row + r], jnp.float32)
        flags = jnp.broadcast_to(flg[pl.ds(first_row + r, 1), :], (8, length))
        alive = 1.0 - flags.astype(jnp.float32)
        link = discount * trace * alive
        level = jnp.where(lane < length - 1, link, 0.0)
        coef = jnp.where(lane < length - 1, link, discount * alive)
        levels = []
        for d in steps:
            levels.append(level)
            level = level * ahead(level, d)
            coef = coef * jnp.where(lane < length - d, ahead(coef, d), 1.0)
        ratio = jnp.exp(newp[r : r + 1, :] - oldp[r : r + 1, :])
        weight = msk[r : r + 1, :].astype(jnp.float32)
        reward = jnp.broadcast_to(rew[pl.ds(first_row + r, 1), :], (8, length))
        following = jnp.where(lane < length - 1, discount * alive, 0.0)
        rows_info.append((trace, levels, coef, ratio, weight, reward, following))
        early[my_slot, r : r + 1, 0:length] = ratio
        early[my_slot, r : r + 1, length : 2 * length] = weight
        early[my_slot, r : r + 1, 2 * length : 3 * length] = coef[0:1, :]
        early[my_slot, r : r + 1, 3 * length : 3 * length + LANES] = jnp.broadcast_to(
            trace[0:1, 0:1] * coef[0:1, 0:1], (1, LANES)
        )

    def row_sums(i):
        def do_chunk(c, _):
            hid_copy(i, c).wait()
            for b in range(chunk // BLOCK):
                rows = pl.ds(pl.multiple_of(c * chunk + b * BLOCK, BLOCK), BLOCK)
                squares = jnp.zeros((BLOCK // 8, 8, LANES), jnp.float32)
                products = jnp.zeros((BLOCK // 8, 8, LANES), jnp.float32)
                for j in range(local_width // LANES):
                    cols = pl.ds(j * LANES, LANES)
                    x = hid[i, rows, cols].astype(jnp.float32).reshape(BLOCK // 8, 8, LANES)
                    squares = squares + x * x
                    products = products + x * scaled[:, cols][None]
                parts[0, rows, :] = squares.reshape(BLOCK, LANES)
                parts[1, rows, :] = products.reshape(BLOCK, LANES)
            return 0

        lax.fori_loop(0, chunks, do_chunk, 0)
        return lane_sums(parts[0]), lane_sums(parts[1])

    for k in range(1, tensor_count):
        for r in range(own_rows):
            squares, products = row_sums((k - 1) * own_rows + r)
            part_send[k - 1, 2 * r : 2 * r + 1, :] = squares[0:1, :]
            part_send[k - 1, 2 * r + 1 : 2 * r + 2, :] = products[0:1, :]

    pl.semaphore_wait(barrier, devices - 1)

    part_copies = []
    for k in range(1, tensor_count):
        copy = pltpu.make_async_remote_copy(
            src_ref=part_send.at[k - 1],
            dst_ref=part_recv.at[k - 1],
            send_sem=part_send_sem.at[k - 1],
            recv_sem=part_recv_sem.at[k - 1],
            device_id=(me_seq, lax.rem(me_ten + k, tensor_count)),
            device_id_type=pl.DeviceIdType.MESH,
        )
        copy.start()
        part_copies.append(copy)

    def send_all(buffer, send_sem, recv_sem):
        def send(k, _):
            pltpu.make_async_remote_copy(
                src_ref=buffer.at[my_slot],
                dst_ref=buffer.at[my_slot],
                send_sem=send_sem,
                recv_sem=recv_sem,
                device_id=peer(k),
                device_id_type=pl.DeviceIdType.MESH,
            ).start()
            return 0

        lax.fori_loop(1, devices, send, 0)

    def all_blocks(buffer, sem):
        view = buffer.at[pl.ds(0, devices - 1)]
        return pltpu.make_async_copy(view, view, sem)

    send_all(early, early_send_sem, early_recv_sem)

    own = [row_sums((tensor_count - 1) * own_rows + r) for r in range(own_rows)]
    for copy in part_copies:
        copy.wait()

    for r in range(own_rows):
        trace, levels, coef, ratio, weight, reward, following = rows_info[r]
        squares, products = own[r]
        for k in range(1, tensor_count):
            squares = squares + part_recv[k - 1, 2 * r : 2 * r + 1, :]
            products = products + part_recv[k - 1, 2 * r + 1 : 2 * r + 2, :]
        values = products * lax.rsqrt(squares / width + EPS_NORM)
        values_ref[r : r + 1, :] = values[0:1, :]
        adv = reward + following * ahead(values, 1) - values
        for d, level in zip(steps, levels):
            adv = adv + level * ahead(adv, d)
        late[my_slot, r : r + 1, 0:length] = adv[0:1, :]
        late[my_slot, r : r + 1, length : length + LANES] = jnp.broadcast_to(
            values[0:1, 0:1] + trace[0:1, 0:1] * adv[0:1, 0:1], (1, LANES)
        )

    send_all(late, late_send_sem, late_recv_sem)

    all_blocks(early, early_recv_sem).wait()
    count = jnp.zeros((seq_count, length), jnp.float32)
    for t in range(tensor_count):
        for r in range(own_rows):
            count = count + early[pl.ds(t * seq_count, seq_count), r, length : 2 * length]
    total = lambda x: jnp.sum(jnp.sum(x, axis=0, keepdims=True), axis=1, keepdims=True)
    count = total(count)
    all_blocks(late, late_recv_sem).wait()

    advs = []
    for t in range(tensor_count):
        for r in range(own_rows):
            entering = jnp.full((1, LANES), boot[t * own_rows + r], jnp.float32)
            for n in range(seq_count - 1, -1, -1):
                slot = t * seq_count + n
                carry[slot, r : r + 1, :] = entering
                if n:
                    offset = late[slot, r : r + 1, length : length + LANES]
                    slope = early[slot, r : r + 1, 3 * length : 3 * length + LANES]
                    entering = offset + slope * entering
    sums = jnp.zeros((seq_count, length), jnp.float32)
    for t in range(tensor_count):
        for r in range(own_rows):
            slots = pl.ds(t * seq_count, seq_count)
            entering = jnp.concatenate([carry[slots, r, :]] * (length // LANES), axis=1)
            adv = late[slots, r, 0:length] + early[slots, r, 2 * length : 3 * length] * entering
            advs.append(adv)
            sums = sums + early[slots, r, length : 2 * length] * adv
    mean = total(sums) / count
    sums = jnp.zeros((seq_count, length), jnp.float32)
    for t in range(tensor_count):
        for r in range(own_rows):
            slots = pl.ds(t * seq_count, seq_count)
            centred = advs[t * own_rows + r] - mean
            advs[t * own_rows + r] = centred
            sums = sums + early[slots, r, length : 2 * length] * centred * centred
    scale = lax.rsqrt(total(sums) / count + EPS_WHITE)

    def token_loss(ratio, weight, white):
        clipped = jnp.clip(ratio, 1.0 - CLIP, 1.0 + CLIP)
        return -weight * jnp.minimum(ratio * white, clipped * white)

    for r in range(own_rows):
        _, _, coef, ratio, weight, _, _ = rows_info[r]
        entering = carry[my_slot, r : r + 1, :]
        entering = jnp.concatenate([entering] * (length // LANES), axis=1)
        adv = late[my_slot, r : r + 1, 0:length] + coef[0:1, :] * entering
        white = (adv - mean) * scale
        white_ref[r : r + 1, :] = white
        token_ref[r : r + 1, :] = token_loss(ratio, weight, white)

    sums = jnp.zeros((seq_count, length), jnp.float32)
    for t in range(tensor_count):
        for r in range(own_rows):
            slots = pl.ds(t * seq_count, seq_count)
            sums = sums + token_loss(
                early[slots, r, 0:length],
                early[slots, r, length : 2 * length],
                advs[t * own_rows + r] * scale,
            )
    loss_ref[...] = jnp.broadcast_to(total(sums) / count, (1, LANES))

    all_blocks(early, early_send_sem).wait()
    all_blocks(late, late_send_sem).wait()


def write_out(*refs):
    half = len(refs) // 2
    for src, dst in zip(refs[:half], refs[half:]):
        dst[...] = src[:, : dst.shape[1]]


def shards(seq_count, tensor_count, *args):
    seqs_all, length, local_width = args[0].shape
    own_rows = seqs_all // tensor_count
    devices = seq_count * tensor_count
    chunk = min(length, 64)
    f32 = jnp.float32
    row = jax.ShapeDtypeStruct((own_rows, length), f32)
    dma = pltpu.SemaphoreType.DMA
    shapes = [row, row, row, jax.ShapeDtypeStruct((1, 1), f32)]
    outs = pl.pallas_call(
        functools.partial(kernel, seq_count, tensor_count, local_width * tensor_count, chunk),
        out_shape=[row, row, row, jax.ShapeDtypeStruct((1, LANES), f32)],
        in_specs=[pl.BlockSpec(memory_space=pltpu.HBM)] * 11,
        out_specs=[pl.BlockSpec(memory_space=pltpu.VMEM)] * 4,
        scratch_shapes=[
            pltpu.VMEM((seqs_all, length, local_width), jnp.bfloat16),
            pltpu.VMEM((local_width,), jnp.bfloat16),
            pltpu.VMEM((local_width,), jnp.bfloat16),
            pltpu.VMEM((seqs_all, length), f32),
            pltpu.VMEM((seqs_all, length), jnp.int32),
            pltpu.VMEM((own_rows, length), jnp.int32),
            pltpu.VMEM((own_rows, length), f32),
            pltpu.VMEM((own_rows, length), f32),
            pltpu.SMEM((seqs_all,), f32),
            pltpu.SMEM((seqs_all,), f32),
            pltpu.SMEM((seqs_all,), f32),
            pltpu.VMEM((8, local_width), f32),
            pltpu.VMEM((2, length, LANES), f32),
            pltpu.VMEM((max(tensor_count - 1, 1), 2 * own_rows, length), f32),
            pltpu.VMEM((max(tensor_count - 1, 1), 2 * own_rows, length), f32),
            pltpu.VMEM((devices, own_rows, 3 * length + LANES), f32),
            pltpu.VMEM((devices, own_rows, length + LANES), f32),
            pltpu.VMEM((devices, own_rows, LANES), f32),
            dma((seqs_all * (length // chunk),)),
            dma((10,)),
            dma((max(tensor_count - 1, 1),)),
            dma((max(tensor_count - 1, 1),)),
            dma,
            dma,
            dma,
            dma,
        ],
        compiler_params=pltpu.CompilerParams(
            collective_id=0, has_side_effects=True, vmem_limit_bytes=24 << 20
        ),
    )(*[pltpu.with_memory_space_constraint(x, pltpu.HBM) for x in args])
    outs = pl.pallas_call(
        write_out,
        out_shape=shapes,
        in_specs=[pl.BlockSpec(memory_space=pltpu.VMEM)] * 4,
        out_specs=[pl.BlockSpec(memory_space=pltpu.VMEM)] * 4,
        compiler_params=pltpu.CompilerParams(vmem_limit_bytes=1 << 20),
    )(*outs)
    return (outs[0], outs[1], outs[2], outs[3].reshape(()))


def solution(mesh):
    in_specs = (
        P(None, "seq", "tensor"),
        P("tensor"),
        P("tensor"),
        P(None, "seq"),
        P(None, "seq"),
        P("tensor", "seq"),
        P("tensor", "seq"),
        P("tensor", "seq"),
        P(),
        P(),
        P(),
    )
    out_specs = (P("tensor", "seq"), P("tensor", "seq"), P("tensor", "seq"), P())
    body = functools.partial(shards, mesh.shape["seq"], mesh.shape["tensor"])
    return jax.shard_map(body, mesh=mesh, in_specs=in_specs, out_specs=out_specs, check_vma=False)
```

```python
import functools

import jax
import jax.numpy as jnp
from jax import lax
from jax.experimental import pallas as pl
from jax.experimental.pallas import tpu as pltpu
from jax.sharding import PartitionSpec as P

EPS_NORM = 1e-06
EPS_WHITE = 1e-08
CLIP = 0.2
HIGHEST = lax.Precision.HIGHEST
LANES = 128
BLOCK = 32


def lane_sums(parts):
    ones = jnp.ones((8, LANES), jnp.float32)
    return lax.dot_general(
        ones, parts, (((1,), (1,)), ((), ())), precision=HIGHEST, preferred_element_type=jnp.float32
    )


def kernel(
    seq_count,
    tensor_count,
    width,
    chunk,
    hidden_hbm,
    gain_hbm,
    weight_hbm,
    rewards_hbm,
    flags_hbm,
    mask_hbm,
    new_hbm,
    old_hbm,
    discount_hbm,
    trace_hbm,
    boot_hbm,
    values_ref,
    white_ref,
    token_ref,
    loss_ref,
    hid,
    gain,
    wgt,
    rew,
    flg,
    msk,
    newp,
    oldp,
    disc,
    trc,
    boot,
    scaled,
    parts,
    part_send,
    part_recv,
    early,
    late,
    carry,
    slope,
    hid_sem,
    in_sem,
    part_send_sem,
    part_recv_sem,
    early_send_sem,
    early_recv_sem,
    late_send_sem,
    late_recv_sem,
):
    seqs_all, length, local_width = hid.shape
    own_rows = seqs_all // tensor_count
    devices = seq_count * tensor_count
    chunks = length // chunk
    me_seq = lax.axis_index("seq")
    me_ten = lax.axis_index("tensor")
    first_row = me_ten * own_rows
    my_slot = me_ten * seq_count + me_seq

    small = [
        (gain_hbm, gain),
        (weight_hbm, wgt),
        (rewards_hbm, rew),
        (flags_hbm, flg),
        (mask_hbm, msk),
        (new_hbm, newp),
        (old_hbm, oldp),
        (discount_hbm, disc),
        (trace_hbm, trc),
        (boot_hbm, boot),
    ]
    small_copies = [
        pltpu.make_async_copy(src, dst, in_sem.at[i]) for i, (src, dst) in enumerate(small)
    ]
    for copy in small_copies:
        copy.start()

    def hid_copy(i, c):
        row = lax.rem(first_row + own_rows + i, seqs_all)
        rows = pl.ds(c * chunk, chunk)
        return pltpu.make_async_copy(
            hidden_hbm.at[row, rows, :], hid.at[i, rows, :], hid_sem.at[i * chunks + c]
        )

    for i in range(seqs_all):
        for c in range(chunks):
            hid_copy(i, c).start()

    barrier = pltpu.get_barrier_semaphore()

    def peer(k):
        slot = lax.rem(my_slot + k, devices)
        return (lax.rem(slot, seq_count), lax.div(slot, seq_count))

    def greet(k, _):
        pl.semaphore_signal(
            barrier, inc=1, device_id=peer(k), device_id_type=pl.DeviceIdType.MESH
        )
        return 0

    lax.fori_loop(1, devices, greet, 0)

    for copy in small_copies:
        copy.wait()

    for j in range(local_width // LANES):
        cols = pl.ds(j * LANES, LANES)
        row = gain[cols].astype(jnp.float32) * wgt[cols].astype(jnp.float32)
        scaled[:, cols] = jnp.broadcast_to(row.reshape(1, LANES), (8, LANES))

    lane = lax.broadcasted_iota(jnp.int32, (8, length), 1)
    steps = []
    step = 1
    while step < length:
        steps.append(step)
        step *= 2
    ahead = lambda x, d: pltpu.roll(x, length - d, 1)
    rows_info = []
    tasks = []

    def scan_task(info, d):
        def run():
            info["levels"].append(info["level"])
            info["level"] = info["level"] * ahead(info["level"], d)

        return run

    def coef_of(last_done, row):
        shape = last_done.shape[:-1] + (length,)
        at = lax.broadcasted_iota(jnp.int32, shape, len(shape) - 1).astype(jnp.float32)
        discount = jnp.full(shape, disc[row], jnp.float32)
        decay = discount * jnp.full(shape, trc[row], jnp.float32)
        power = jnp.exp((length - 1.0 - at) * jnp.log(decay))
        return jnp.where(at > last_done[..., 0:1], discount * power, 0.0)

    for r in range(own_rows):
        discount = jnp.full((8, length), disc[first_row + r], jnp.float32)
        trace = jnp.full((8, length), trc[first_row + r], jnp.float32)
        flags = jnp.broadcast_to(flg[pl.ds(first_row + r, 1), :], (8, length))
        alive = 1.0 - flags.astype(jnp.float32)
        ratio = jnp.exp(newp[r : r + 1, :] - oldp[r : r + 1, :])
        weight = msk[r : r + 1, :].astype(jnp.float32)
        reward = jnp.broadcast_to(rew[pl.ds(first_row + r, 1), :], (8, length))
        last_done = jnp.max(
            jnp.where(flags > 0, lane, -1).astype(jnp.float32)[0:1, :], axis=1, keepdims=True
        )
        info = dict(
            trace=trace,
            level=jnp.where(lane < length - 1, discount * trace * alive, 0.0),
            levels=[],
            ratio=ratio,
            weight=weight,
            reward=reward,
            following=jnp.where(lane < length - 1, discount * alive, 0.0),
        )
        rows_info.append(info)
        tasks += [scan_task(info, d) for d in steps]
        early[my_slot, r : r + 1, 0:length] = ratio
        early[my_slot, r : r + 1, length : 2 * length] = weight
        early[my_slot, r : r + 1, 2 * length : 2 * length + LANES] = jnp.broadcast_to(
            last_done, (1, LANES)
        )
    all_chunks = seqs_all * chunks
    task_count = len(tasks)

    def row_sums(i):
        for c in range(chunks):
            g = i * chunks + c
            hid_copy(i, c).wait()
            for task in tasks[g * task_count // all_chunks : (g + 1) * task_count // all_chunks]:
                task()
            for b in range(chunk // BLOCK):
                rows = pl.ds(c * chunk + b * BLOCK, BLOCK)
                squares = jnp.zeros((BLOCK // 8, 8, LANES), jnp.float32)
                products = jnp.zeros((BLOCK // 8, 8, LANES), jnp.float32)
                for j in range(local_width // LANES):
                    cols = pl.ds(j * LANES, LANES)
                    x = hid[i, rows, cols].astype(jnp.float32).reshape(BLOCK // 8, 8, LANES)
                    squares = squares + x * x
                    products = products + x * scaled[:, cols][None]
                parts[0, rows, :] = squares.reshape(BLOCK, LANES)
                parts[1, rows, :] = products.reshape(BLOCK, LANES)
        return lane_sums(parts[0]), lane_sums(parts[1])

    for k in range(1, tensor_count):
        for r in range(own_rows):
            squares, products = row_sums((k - 1) * own_rows + r)
            part_send[k - 1, 2 * r : 2 * r + 1, :] = squares[0:1, :]
            part_send[k - 1, 2 * r + 1 : 2 * r + 2, :] = products[0:1, :]

    pl.semaphore_wait(barrier, devices - 1)

    part_copies = []
    for k in range(1, tensor_count):
        copy = pltpu.make_async_remote_copy(
            src_ref=part_send.at[k - 1],
            dst_ref=part_recv.at[k - 1],
            send_sem=part_send_sem.at[k - 1],
            recv_sem=part_recv_sem.at[k - 1],
            device_id=(me_seq, lax.rem(me_ten + k, tensor_count)),
            device_id_type=pl.DeviceIdType.MESH,
        )
        copy.start()
        part_copies.append(copy)

    def send_all(buffer, send_sem, recv_sem):
        def send(k, _):
            pltpu.make_async_remote_copy(
                src_ref=buffer.at[my_slot],
                dst_ref=buffer.at[my_slot],
                send_sem=send_sem,
                recv_sem=recv_sem,
                device_id=peer(k),
                device_id_type=pl.DeviceIdType.MESH,
            ).start()
            return 0

        lax.fori_loop(1, devices, send, 0)

    def all_blocks(buffer, sem):
        view = buffer.at[pl.ds(0, devices - 1)]
        return pltpu.make_async_copy(view, view, sem)

    send_all(early, early_send_sem, early_recv_sem)

    own = [row_sums((tensor_count - 1) * own_rows + r) for r in range(own_rows)]
    for copy in part_copies:
        copy.wait()

    for r in range(own_rows):
        info = rows_info[r]
        trace, levels, reward, following = (
            info[name] for name in ("trace", "levels", "reward", "following")
        )
        squares, products = own[r]
        for k in range(1, tensor_count):
            squares = squares + part_recv[k - 1, 2 * r : 2 * r + 1, :]
            products = products + part_recv[k - 1, 2 * r + 1 : 2 * r + 2, :]
        values = products * lax.rsqrt(squares / width + EPS_NORM)
        values_ref[r : r + 1, :] = values[0:1, :]
        adv = reward + following * ahead(values, 1) - values
        for d, level in zip(steps, levels):
            adv = adv + level * ahead(adv, d)
        late[my_slot, r : r + 1, 0:length] = adv[0:1, :]
        late[my_slot, r : r + 1, length : length + LANES] = jnp.broadcast_to(
            values[0:1, 0:1] + trace[0:1, 0:1] * adv[0:1, 0:1], (1, LANES)
        )

    send_all(late, late_send_sem, late_recv_sem)

    all_blocks(early, early_recv_sem).wait()
    count = jnp.zeros((seq_count, length), jnp.float32)
    for t in range(tensor_count):
        for r in range(own_rows):
            count = count + early[pl.ds(t * seq_count, seq_count), r, length : 2 * length]
    total = lambda x: jnp.sum(jnp.sum(x, axis=0, keepdims=True), axis=1, keepdims=True)
    count = total(count)
    coefs = []
    for t in range(tensor_count):
        for r in range(own_rows):
            row = t * own_rows + r
            slots = pl.ds(t * seq_count, seq_count)
            coef = coef_of(early[slots, r, 2 * length : 2 * length + LANES], row)
            coefs.append(coef)
            slope[slots, r, :] = jnp.broadcast_to(trc[row] * coef[:, 0:1], (seq_count, LANES))
    all_blocks(late, late_recv_sem).wait()

    advs = []
    for t in range(tensor_count):
        for r in range(own_rows):
            entering = jnp.full((1, LANES), boot[t * own_rows + r], jnp.float32)
            for n in range(seq_count - 1, -1, -1):
                slot = t * seq_count + n
                carry[slot, r : r + 1, :] = entering
                if n:
                    offset = late[slot, r : r + 1, length : length + LANES]
                    entering = offset + slope[slot, r : r + 1, :] * entering
    sums = jnp.zeros((seq_count, length), jnp.float32)
    for t in range(tensor_count):
        for r in range(own_rows):
            slots = pl.ds(t * seq_count, seq_count)
            entering = jnp.concatenate([carry[slots, r, :]] * (length // LANES), axis=1)
            adv = late[slots, r, 0:length] + coefs[t * own_rows + r] * entering
            advs.append(adv)
            sums = sums + early[slots, r, length : 2 * length] * adv
    mean = total(sums) / count
    sums = jnp.zeros((seq_count, length), jnp.float32)
    for t in range(tensor_count):
        for r in range(own_rows):
            slots = pl.ds(t * seq_count, seq_count)
            centred = advs[t * own_rows + r] - mean
            advs[t * own_rows + r] = centred
            sums = sums + early[slots, r, length : 2 * length] * centred * centred
    scale = lax.rsqrt(total(sums) / count + EPS_WHITE)

    def token_loss(ratio, weight, white):
        clipped = jnp.clip(ratio, 1.0 - CLIP, 1.0 + CLIP)
        return -weight * jnp.minimum(ratio * white, clipped * white)

    for r in range(own_rows):
        ratio, weight = rows_info[r]["ratio"], rows_info[r]["weight"]
        coef = coef_of(early[my_slot, r : r + 1, 2 * length : 2 * length + LANES], first_row + r)
        entering = carry[my_slot, r : r + 1, :]
        entering = jnp.concatenate([entering] * (length // LANES), axis=1)
        adv = late[my_slot, r : r + 1, 0:length] + coef * entering
        white = (adv - mean) * scale
        white_ref[r : r + 1, :] = white
        token_ref[r : r + 1, :] = token_loss(ratio, weight, white)

    sums = jnp.zeros((seq_count, length), jnp.float32)
    for t in range(tensor_count):
        for r in range(own_rows):
            slots = pl.ds(t * seq_count, seq_count)
            sums = sums + token_loss(
                early[slots, r, 0:length],
                early[slots, r, length : 2 * length],
                advs[t * own_rows + r] * scale,
            )
    loss_ref[...] = jnp.broadcast_to(total(sums) / count, (1, LANES))

    all_blocks(early, early_send_sem).wait()
    all_blocks(late, late_send_sem).wait()


def write_out(*refs):
    half = len(refs) // 2
    for src, dst in zip(refs[:half], refs[half:]):
        dst[...] = src[:, : dst.shape[1]]


def shards(seq_count, tensor_count, *args):
    seqs_all, length, local_width = args[0].shape
    own_rows = seqs_all // tensor_count
    devices = seq_count * tensor_count
    chunk = min(length, 64)
    f32 = jnp.float32
    row = jax.ShapeDtypeStruct((own_rows, length), f32)
    dma = pltpu.SemaphoreType.DMA
    shapes = [row, row, row, jax.ShapeDtypeStruct((1, 1), f32)]
    outs = pl.pallas_call(
        functools.partial(kernel, seq_count, tensor_count, local_width * tensor_count, chunk),
        out_shape=[row, row, row, jax.ShapeDtypeStruct((1, LANES), f32)],
        in_specs=[pl.BlockSpec(memory_space=pltpu.HBM)] * 11,
        out_specs=[pl.BlockSpec(memory_space=pltpu.VMEM)] * 4,
        scratch_shapes=[
            pltpu.VMEM((seqs_all, length, local_width), jnp.bfloat16),
            pltpu.VMEM((local_width,), jnp.bfloat16),
            pltpu.VMEM((local_width,), jnp.bfloat16),
            pltpu.VMEM((seqs_all, length), f32),
            pltpu.VMEM((seqs_all, length), jnp.int32),
            pltpu.VMEM((own_rows, length), jnp.int32),
            pltpu.VMEM((own_rows, length), f32),
            pltpu.VMEM((own_rows, length), f32),
            pltpu.SMEM((seqs_all,), f32),
            pltpu.SMEM((seqs_all,), f32),
            pltpu.SMEM((seqs_all,), f32),
            pltpu.VMEM((8, local_width), f32),
            pltpu.VMEM((2, length, LANES), f32),
            pltpu.VMEM((max(tensor_count - 1, 1), 2 * own_rows, length), f32),
            pltpu.VMEM((max(tensor_count - 1, 1), 2 * own_rows, length), f32),
            pltpu.VMEM((devices, own_rows, 2 * length + LANES), f32),
            pltpu.VMEM((devices, own_rows, length + LANES), f32),
            pltpu.VMEM((devices, own_rows, LANES), f32),
            pltpu.VMEM((devices, own_rows, LANES), f32),
            dma((seqs_all * (length // chunk),)),
            dma((10,)),
            dma((max(tensor_count - 1, 1),)),
            dma((max(tensor_count - 1, 1),)),
            dma,
            dma,
            dma,
            dma,
        ],
        compiler_params=pltpu.CompilerParams(
            collective_id=0, has_side_effects=True, vmem_limit_bytes=24 << 20
        ),
    )(*[pltpu.with_memory_space_constraint(x, pltpu.HBM) for x in args])
    outs = pl.pallas_call(
        write_out,
        out_shape=shapes,
        in_specs=[pl.BlockSpec(memory_space=pltpu.VMEM)] * 4,
        out_specs=[pl.BlockSpec(memory_space=pltpu.VMEM)] * 4,
        compiler_params=pltpu.CompilerParams(vmem_limit_bytes=1 << 20),
    )(*outs)
    return (outs[0], outs[1], outs[2], outs[3].reshape(()))


def solution(mesh):
    in_specs = (
        P(None, "seq", "tensor"),
        P("tensor"),
        P("tensor"),
        P(None, "seq"),
        P(None, "seq"),
        P("tensor", "seq"),
        P("tensor", "seq"),
        P("tensor", "seq"),
        P(),
        P(),
        P(),
    )
    out_specs = (P("tensor", "seq"), P("tensor", "seq"), P("tensor", "seq"), P())
    body = functools.partial(shards, mesh.shape["seq"], mesh.shape["tensor"])
    return jax.shard_map(body, mesh=mesh, in_specs=in_specs, out_specs=out_specs, check_vma=False)
```

```python
import functools

import jax
import jax.numpy as jnp
from jax import lax
from jax.experimental import pallas as pl
from jax.experimental.pallas import tpu as pltpu
from jax.sharding import PartitionSpec as P

EPS_NORM = 1e-06
EPS_WHITE = 1e-08
CLIP = 0.2
LANES = 128
BLOCK = 32
UNROLLED = 64


def lane_sums(parts):
    total = 0.0
    for _ in range(3):
        piece = parts.astype(jnp.bfloat16)
        parts = parts - piece.astype(jnp.float32)
        total = total + lax.dot_general(
            jnp.ones((8, LANES), jnp.bfloat16),
            piece,
            (((1,), (1,)), ((), ())),
            preferred_element_type=jnp.float32,
        )
    return total


def kernel(
    seq_count,
    tensor_count,
    width,
    chunk,
    hidden_hbm,
    gain_hbm,
    weight_hbm,
    rewards_hbm,
    flags_hbm,
    mask_hbm,
    new_hbm,
    old_hbm,
    discount_hbm,
    trace_hbm,
    boot_hbm,
    values_ref,
    white_ref,
    token_ref,
    loss_ref,
    hid,
    gain,
    wgt,
    rew,
    flg,
    msk,
    newp,
    oldp,
    disc,
    trc,
    boot,
    scaled,
    parts,
    part_send,
    part_recv,
    early,
    late,
    carry,
    slope,
    hid_sem,
    in_sem,
    part_send_sem,
    part_recv_sem,
    early_send_sem,
    early_recv_sem,
    late_send_sem,
    late_recv_sem,
):
    seqs_all, length, local_width = hid.shape
    own_rows = seqs_all // tensor_count
    devices = seq_count * tensor_count
    chunks = length // chunk
    me_seq = lax.axis_index("seq")
    me_ten = lax.axis_index("tensor")
    first_row = me_ten * own_rows
    my_slot = me_ten * seq_count + me_seq

    small = [
        (gain_hbm, gain),
        (weight_hbm, wgt),
        (rewards_hbm, rew),
        (flags_hbm, flg),
        (mask_hbm, msk),
        (new_hbm, newp),
        (old_hbm, oldp),
        (discount_hbm, disc),
        (trace_hbm, trc),
        (boot_hbm, boot),
    ]
    small_copies = [
        pltpu.make_async_copy(src, dst, in_sem.at[i]) for i, (src, dst) in enumerate(small)
    ]
    for copy in small_copies:
        copy.start()

    def hid_copy(i, c):
        row = lax.rem(first_row + own_rows + i, seqs_all)
        rows = pl.ds(c * chunk, chunk)
        return pltpu.make_async_copy(
            hidden_hbm.at[row, rows, :], hid.at[i, rows, :], hid_sem.at[i * chunks + c]
        )

    for i in range(seqs_all):
        for c in range(chunks):
            hid_copy(i, c).start()

    barrier = pltpu.get_barrier_semaphore()

    def peer(k):
        slot = lax.rem(my_slot + k, devices)
        return (lax.rem(slot, seq_count), lax.div(slot, seq_count))

    def each_peer(act):
        if devices <= UNROLLED:
            for k in range(1, devices):
                act(k, 0)
        else:
            lax.fori_loop(1, devices, act, 0)

    def greet(k, _):
        pl.semaphore_signal(
            barrier, inc=1, device_id=peer(k), device_id_type=pl.DeviceIdType.MESH
        )
        return 0

    each_peer(greet)

    for copy in small_copies:
        copy.wait()

    for j in range(local_width // LANES):
        cols = pl.ds(j * LANES, LANES)
        row = gain[cols].astype(jnp.float32) * wgt[cols].astype(jnp.float32)
        scaled[:, cols] = jnp.broadcast_to(row.reshape(1, LANES), (8, LANES))

    lane = lax.broadcasted_iota(jnp.int32, (8, length), 1)
    steps = []
    step = 1
    while step < length:
        steps.append(step)
        step *= 4
    ahead = lambda x, d: pltpu.roll(x, (length - d) % length, 1)
    rows_info = []
    tasks = []

    def scan_task(info, d):
        def run():
            one = info["level"]
            two = one * ahead(one, d)
            info["levels"] += [(d, one), (2 * d, two), (3 * d, one * ahead(two, d))]
            info["level"] = two * ahead(two, 2 * d)

        return run

    def coef_of(last_done, row):
        shape = last_done.shape[:-1] + (length,)
        at = lax.broadcasted_iota(jnp.int32, shape, len(shape) - 1).astype(jnp.float32)
        discount = jnp.full(shape, disc[row], jnp.float32)
        decay = discount * jnp.full(shape, trc[row], jnp.float32)
        power = jnp.exp((length - 1.0 - at) * jnp.log(decay))
        return jnp.where(at > last_done[..., 0:1], discount * power, 0.0)

    for r in range(own_rows):
        discount = jnp.full((8, length), disc[first_row + r], jnp.float32)
        trace = jnp.full((8, length), trc[first_row + r], jnp.float32)
        flags = jnp.broadcast_to(flg[pl.ds(first_row + r, 1), :], (8, length))
        alive = 1.0 - flags.astype(jnp.float32)
        ratio = jnp.exp(newp[r : r + 1, :] - oldp[r : r + 1, :])
        weight = msk[r : r + 1, :].astype(jnp.float32)
        reward = jnp.broadcast_to(rew[pl.ds(first_row + r, 1), :], (8, length))
        last_done = jnp.max(
            jnp.where(flags > 0, lane, -1).astype(jnp.float32)[0:1, :], axis=1, keepdims=True
        )
        info = dict(
            trace=trace,
            level=jnp.where(lane < length - 1, discount * trace * alive, 0.0),
            levels=[],
            ratio=ratio,
            weight=weight,
            reward=reward,
            following=jnp.where(lane < length - 1, discount * alive, 0.0),
        )
        rows_info.append(info)
        tasks += [scan_task(info, d) for d in steps]
        early[my_slot, r : r + 1, 0:length] = ratio
        early[my_slot, r : r + 1, length : 2 * length] = weight
        early[my_slot, r : r + 1, 2 * length : 2 * length + LANES] = jnp.broadcast_to(
            last_done, (1, LANES)
        )
    all_chunks = seqs_all * chunks
    task_count = len(tasks)

    def row_sums(i):
        start, squares_rows, products_rows = 0, [], []
        for c in range(chunks):
            g = i * chunks + c
            hid_copy(i, c).wait()
            for task in tasks[g * task_count // all_chunks : (g + 1) * task_count // all_chunks]:
                task()
            for b in range(chunk // BLOCK):
                rows = pl.ds(c * chunk + b * BLOCK, BLOCK)
                squares = jnp.zeros((BLOCK // 8, 8, LANES), jnp.float32)
                products = jnp.zeros((BLOCK // 8, 8, LANES), jnp.float32)
                for j in range(local_width // LANES):
                    cols = pl.ds(j * LANES, LANES)
                    x = hid[i, rows, cols].astype(jnp.float32).reshape(BLOCK // 8, 8, LANES)
                    squares = squares + x * x
                    products = products + x * scaled[:, cols][None]
                parts[0, rows, :] = squares.reshape(BLOCK, LANES)
                parts[1, rows, :] = products.reshape(BLOCK, LANES)
            done = (c + 1) * chunk
            if done % LANES == 0 or done == length:
                rows = pl.ds(start, done - start)
                squares_rows.append(lane_sums(parts[0, rows, :]))
                products_rows.append(lane_sums(parts[1, rows, :]))
                start = done
        return jnp.concatenate(squares_rows, axis=1), jnp.concatenate(products_rows, axis=1)

    for k in range(1, tensor_count):
        for r in range(own_rows):
            squares, products = row_sums((k - 1) * own_rows + r)
            part_send[k - 1, 2 * r : 2 * r + 1, :] = squares[0:1, :]
            part_send[k - 1, 2 * r + 1 : 2 * r + 2, :] = products[0:1, :]

    pl.semaphore_wait(barrier, devices - 1)

    part_copies = []
    for k in range(1, tensor_count):
        copy = pltpu.make_async_remote_copy(
            src_ref=part_send.at[k - 1],
            dst_ref=part_recv.at[k - 1],
            send_sem=part_send_sem.at[k - 1],
            recv_sem=part_recv_sem.at[k - 1],
            device_id=(me_seq, lax.rem(me_ten + k, tensor_count)),
            device_id_type=pl.DeviceIdType.MESH,
        )
        copy.start()
        part_copies.append(copy)

    def send_all(buffer, send_sem, recv_sem):
        def send(k, _):
            pltpu.make_async_remote_copy(
                src_ref=buffer.at[my_slot],
                dst_ref=buffer.at[my_slot],
                send_sem=send_sem,
                recv_sem=recv_sem,
                device_id=peer(k),
                device_id_type=pl.DeviceIdType.MESH,
            ).start()
            return 0

        each_peer(send)

    def all_blocks(buffer, sem):
        view = buffer.at[pl.ds(0, devices - 1)]
        return pltpu.make_async_copy(view, view, sem)

    send_all(early, early_send_sem, early_recv_sem)

    own = [row_sums((tensor_count - 1) * own_rows + r) for r in range(own_rows)]
    for copy in part_copies:
        copy.wait()

    for r in range(own_rows):
        info = rows_info[r]
        trace, levels, reward, following = (
            info[name] for name in ("trace", "levels", "reward", "following")
        )
        squares, products = own[r]
        for k in range(1, tensor_count):
            squares = squares + part_recv[k - 1, 2 * r : 2 * r + 1, :]
            products = products + part_recv[k - 1, 2 * r + 1 : 2 * r + 2, :]
        values = products * lax.rsqrt(squares / width + EPS_NORM)
        values_ref[r : r + 1, :] = values[0:1, :]
        adv = reward + following * ahead(values, 1) - values
        for n in range(0, len(levels), 3):
            adv = adv + sum(level * ahead(adv, d) for d, level in levels[n : n + 3] if d < length)
        late[my_slot, r : r + 1, 0:length] = adv[0:1, :]
        late[my_slot, r : r + 1, length : length + LANES] = jnp.broadcast_to(
            values[0:1, 0:1] + trace[0:1, 0:1] * adv[0:1, 0:1], (1, LANES)
        )

    send_all(late, late_send_sem, late_recv_sem)

    all_blocks(early, early_recv_sem).wait()
    count = jnp.zeros((seq_count, length), jnp.float32)
    for t in range(tensor_count):
        for r in range(own_rows):
            count = count + early[pl.ds(t * seq_count, seq_count), r, length : 2 * length]
    total = lambda x: jnp.sum(jnp.sum(x, axis=0, keepdims=True), axis=1, keepdims=True)
    count = total(count)
    coefs = []
    for t in range(tensor_count):
        for r in range(own_rows):
            row = t * own_rows + r
            slots = pl.ds(t * seq_count, seq_count)
            coef = coef_of(early[slots, r, 2 * length : 2 * length + LANES], row)
            coefs.append(coef)
            slope[slots, r, :] = jnp.broadcast_to(trc[row] * coef[:, 0:1], (seq_count, LANES))
    all_blocks(late, late_recv_sem).wait()

    advs = []
    for t in range(tensor_count):
        for r in range(own_rows):
            entering = jnp.full((1, LANES), boot[t * own_rows + r], jnp.float32)
            for n in range(seq_count - 1, -1, -1):
                slot = t * seq_count + n
                carry[slot, r : r + 1, :] = entering
                if n:
                    offset = late[slot, r : r + 1, length : length + LANES]
                    entering = offset + slope[slot, r : r + 1, :] * entering
    sums = jnp.zeros((seq_count, length), jnp.float32)
    for t in range(tensor_count):
        for r in range(own_rows):
            slots = pl.ds(t * seq_count, seq_count)
            entering = jnp.concatenate([carry[slots, r, :]] * (length // LANES), axis=1)
            adv = late[slots, r, 0:length] + coefs[t * own_rows + r] * entering
            advs.append(adv)
            sums = sums + early[slots, r, length : 2 * length] * adv
    mean = total(sums) / count
    sums = jnp.zeros((seq_count, length), jnp.float32)
    for t in range(tensor_count):
        for r in range(own_rows):
            slots = pl.ds(t * seq_count, seq_count)
            centred = advs[t * own_rows + r] - mean
            advs[t * own_rows + r] = centred
            sums = sums + early[slots, r, length : 2 * length] * centred * centred
    scale = lax.rsqrt(total(sums) / count + EPS_WHITE)

    def token_loss(ratio, weight, white):
        clipped = jnp.clip(ratio, 1.0 - CLIP, 1.0 + CLIP)
        return -weight * jnp.minimum(ratio * white, clipped * white)

    for r in range(own_rows):
        ratio, weight = rows_info[r]["ratio"], rows_info[r]["weight"]
        coef = coef_of(early[my_slot, r : r + 1, 2 * length : 2 * length + LANES], first_row + r)
        entering = carry[my_slot, r : r + 1, :]
        entering = jnp.concatenate([entering] * (length // LANES), axis=1)
        adv = late[my_slot, r : r + 1, 0:length] + coef * entering
        white = (adv - mean) * scale
        white_ref[r : r + 1, :] = white
        token_ref[r : r + 1, :] = token_loss(ratio, weight, white)

    sums = jnp.zeros((seq_count, length), jnp.float32)
    for t in range(tensor_count):
        for r in range(own_rows):
            slots = pl.ds(t * seq_count, seq_count)
            sums = sums + token_loss(
                early[slots, r, 0:length],
                early[slots, r, length : 2 * length],
                advs[t * own_rows + r] * scale,
            )
    loss_ref[...] = jnp.broadcast_to(total(sums) / count, (1, LANES))

    all_blocks(early, early_send_sem).wait()
    all_blocks(late, late_send_sem).wait()


def write_out(*refs):
    half = len(refs) // 2
    for src, dst in zip(refs[:half], refs[half:]):
        dst[...] = src[:, : dst.shape[1]]


def shards(seq_count, tensor_count, *args):
    seqs_all, length, local_width = args[0].shape
    own_rows = seqs_all // tensor_count
    devices = seq_count * tensor_count
    chunk = min(length, 64)
    f32 = jnp.float32
    row = jax.ShapeDtypeStruct((own_rows, length), f32)
    dma = pltpu.SemaphoreType.DMA
    shapes = [row, row, row, jax.ShapeDtypeStruct((1, 1), f32)]
    outs = pl.pallas_call(
        functools.partial(kernel, seq_count, tensor_count, local_width * tensor_count, chunk),
        out_shape=[row, row, row, jax.ShapeDtypeStruct((1, LANES), f32)],
        in_specs=[pl.BlockSpec(memory_space=pltpu.HBM)] * 11,
        out_specs=[pl.BlockSpec(memory_space=pltpu.VMEM)] * 4,
        scratch_shapes=[
            pltpu.VMEM((seqs_all, length, local_width), jnp.bfloat16),
            pltpu.VMEM((local_width,), jnp.bfloat16),
            pltpu.VMEM((local_width,), jnp.bfloat16),
            pltpu.VMEM((seqs_all, length), f32),
            pltpu.VMEM((seqs_all, length), jnp.int32),
            pltpu.VMEM((own_rows, length), jnp.int32),
            pltpu.VMEM((own_rows, length), f32),
            pltpu.VMEM((own_rows, length), f32),
            pltpu.SMEM((seqs_all,), f32),
            pltpu.SMEM((seqs_all,), f32),
            pltpu.SMEM((seqs_all,), f32),
            pltpu.VMEM((8, local_width), f32),
            pltpu.VMEM((2, length, LANES), f32),
            pltpu.VMEM((max(tensor_count - 1, 1), 2 * own_rows, length), f32),
            pltpu.VMEM((max(tensor_count - 1, 1), 2 * own_rows, length), f32),
            pltpu.VMEM((devices, own_rows, 2 * length + LANES), f32),
            pltpu.VMEM((devices, own_rows, length + LANES), f32),
            pltpu.VMEM((devices, own_rows, LANES), f32),
            pltpu.VMEM((devices, own_rows, LANES), f32),
            dma((seqs_all * (length // chunk),)),
            dma((10,)),
            dma((max(tensor_count - 1, 1),)),
            dma((max(tensor_count - 1, 1),)),
            dma,
            dma,
            dma,
            dma,
        ],
        compiler_params=pltpu.CompilerParams(
            collective_id=0, has_side_effects=True, vmem_limit_bytes=24 << 20
        ),
    )(*[pltpu.with_memory_space_constraint(x, pltpu.HBM) for x in args])
    outs = pl.pallas_call(
        write_out,
        out_shape=shapes,
        in_specs=[pl.BlockSpec(memory_space=pltpu.VMEM)] * 4,
        out_specs=[pl.BlockSpec(memory_space=pltpu.VMEM)] * 4,
        compiler_params=pltpu.CompilerParams(vmem_limit_bytes=1 << 20),
    )(*outs)
    return (outs[0], outs[1], outs[2], outs[3].reshape(()))


def solution(mesh):
    in_specs = (
        P(None, "seq", "tensor"),
        P("tensor"),
        P("tensor"),
        P(None, "seq"),
        P(None, "seq"),
        P("tensor", "seq"),
        P("tensor", "seq"),
        P("tensor", "seq"),
        P(),
        P(),
        P(),
    )
    out_specs = (P("tensor", "seq"), P("tensor", "seq"), P("tensor", "seq"), P())
    body = functools.partial(shards, mesh.shape["seq"], mesh.shape["tensor"])
    return jax.shard_map(body, mesh=mesh, in_specs=in_specs, out_specs=out_specs, check_vma=False)
```

```python
import functools

import jax
import jax.numpy as jnp
from jax import lax
from jax.experimental import pallas as pl
from jax.experimental.pallas import tpu as pltpu
from jax.sharding import PartitionSpec as P

EPS_NORM = 1e-06
EPS_WHITE = 1e-08
CLIP = 0.2
LANES = 128
BLOCK = 32
UNROLLED = 64
IN_FLIGHT = 4


def lane_sums(parts):
    total = 0.0
    for _ in range(3):
        piece = parts.astype(jnp.bfloat16)
        parts = parts - piece.astype(jnp.float32)
        total = total + lax.dot_general(
            jnp.ones((8, LANES), jnp.bfloat16),
            piece,
            (((1,), (1,)), ((), ())),
            preferred_element_type=jnp.float32,
        )
    return total


def kernel(
    seq_count,
    tensor_count,
    width,
    chunk,
    hidden_hbm,
    gain_hbm,
    weight_hbm,
    rewards_hbm,
    flags_hbm,
    mask_hbm,
    new_hbm,
    old_hbm,
    discount_hbm,
    trace_hbm,
    boot_hbm,
    values_ref,
    white_ref,
    token_ref,
    loss_ref,
    hid,
    gain,
    wgt,
    rew,
    flg,
    msk,
    newp,
    oldp,
    disc,
    trc,
    boot,
    scaled,
    parts,
    part_send,
    part_recv,
    early,
    late,
    carry,
    slope,
    hid_sem,
    in_sem,
    part_send_sem,
    part_recv_sem,
    early_send_sem,
    early_recv_sem,
    late_send_sem,
    late_recv_sem,
):
    seqs_all, length, local_width = hid.shape
    own_rows = seqs_all // tensor_count
    devices = seq_count * tensor_count
    chunks = length // chunk
    me_seq = lax.axis_index("seq")
    me_ten = lax.axis_index("tensor")
    first_row = me_ten * own_rows
    my_slot = me_ten * seq_count + me_seq

    small = [
        (gain_hbm, gain),
        (weight_hbm, wgt),
        (rewards_hbm, rew),
        (flags_hbm, flg),
        (mask_hbm, msk),
        (new_hbm, newp),
        (old_hbm, oldp),
        (discount_hbm, disc),
        (trace_hbm, trc),
        (boot_hbm, boot),
    ]
    small_copies = [
        pltpu.make_async_copy(src, dst, in_sem.at[i]) for i, (src, dst) in enumerate(small)
    ]
    for copy in small_copies:
        copy.start()

    def hid_copy(i, c):
        row = lax.rem(first_row + own_rows + i, seqs_all)
        rows = pl.ds(c * chunk, chunk)
        return pltpu.make_async_copy(
            hidden_hbm.at[row, rows, :], hid.at[i, rows, :], hid_sem.at[i * chunks + c]
        )

    for g in range(min(IN_FLIGHT, seqs_all * chunks)):
        hid_copy(g // chunks, g % chunks).start()

    barrier = pltpu.get_barrier_semaphore()

    def peer(k):
        slot = lax.rem(my_slot + k, devices)
        return (lax.rem(slot, seq_count), lax.div(slot, seq_count))

    def each_peer(act):
        if devices <= UNROLLED:
            for k in range(1, devices):
                act(k, 0)
        else:
            lax.fori_loop(1, devices, act, 0)

    def greet(k, _):
        pl.semaphore_signal(
            barrier, inc=1, device_id=peer(k), device_id_type=pl.DeviceIdType.MESH
        )
        return 0

    each_peer(greet)

    for copy in small_copies:
        copy.wait()

    for j in range(local_width // LANES):
        cols = pl.ds(j * LANES, LANES)
        row = gain[cols].astype(jnp.float32) * wgt[cols].astype(jnp.float32)
        scaled[:, cols] = jnp.broadcast_to(row.reshape(1, LANES), (8, LANES))

    lane = lax.broadcasted_iota(jnp.int32, (8, length), 1)
    steps = []
    step = 1
    while step < length:
        steps.append(step)
        step *= 4
    ahead = lambda x, d: pltpu.roll(x, (length - d) % length, 1)
    rows_info = []
    tasks = []

    def scan_task(info, d):
        def run():
            one = info["level"]
            two = one * ahead(one, d)
            info["levels"] += [(d, one), (2 * d, two), (3 * d, one * ahead(two, d))]
            info["level"] = two * ahead(two, 2 * d)

        return run

    def coef_of(last_done, row):
        shape = last_done.shape[:-1] + (length,)
        at = lax.broadcasted_iota(jnp.int32, shape, len(shape) - 1).astype(jnp.float32)
        discount = jnp.full(shape, disc[row], jnp.float32)
        decay = discount * jnp.full(shape, trc[row], jnp.float32)
        power = jnp.exp((length - 1.0 - at) * jnp.log(decay))
        return jnp.where(at > last_done[..., 0:1], discount * power, 0.0)

    for r in range(own_rows):
        discount = jnp.full((8, length), disc[first_row + r], jnp.float32)
        trace = jnp.full((8, length), trc[first_row + r], jnp.float32)
        flags = jnp.broadcast_to(flg[pl.ds(first_row + r, 1), :], (8, length))
        alive = 1.0 - flags.astype(jnp.float32)
        ratio = jnp.exp(newp[r : r + 1, :] - oldp[r : r + 1, :])
        weight = msk[r : r + 1, :].astype(jnp.float32)
        reward = jnp.broadcast_to(rew[pl.ds(first_row + r, 1), :], (8, length))
        last_done = jnp.max(
            jnp.where(flags > 0, lane, -1).astype(jnp.float32)[0:1, :], axis=1, keepdims=True
        )
        info = dict(
            trace=trace,
            level=jnp.where(lane < length - 1, discount * trace * alive, 0.0),
            levels=[],
            ratio=ratio,
            weight=weight,
            reward=reward,
            following=jnp.where(lane < length - 1, discount * alive, 0.0),
        )
        rows_info.append(info)
        tasks += [scan_task(info, d) for d in steps]
        early[my_slot, r : r + 1, 0:length] = ratio
        early[my_slot, r : r + 1, length : 2 * length] = weight
        early[my_slot, r : r + 1, 2 * length : 2 * length + LANES] = jnp.broadcast_to(
            last_done, (1, LANES)
        )
    all_chunks = seqs_all * chunks
    task_count = len(tasks)

    def row_sums(i):
        start, squares_rows, products_rows = 0, [], []
        for c in range(chunks):
            g = i * chunks + c
            hid_copy(i, c).wait()
            if g + IN_FLIGHT < all_chunks:
                hid_copy((g + IN_FLIGHT) // chunks, (g + IN_FLIGHT) % chunks).start()
            for task in tasks[g * task_count // all_chunks : (g + 1) * task_count // all_chunks]:
                task()
            for b in range(chunk // BLOCK):
                rows = pl.ds(c * chunk + b * BLOCK, BLOCK)
                squares = jnp.zeros((BLOCK // 8, 8, LANES), jnp.float32)
                products = jnp.zeros((BLOCK // 8, 8, LANES), jnp.float32)
                for j in range(local_width // LANES):
                    cols = pl.ds(j * LANES, LANES)
                    x = hid[i, rows, cols].astype(jnp.float32).reshape(BLOCK // 8, 8, LANES)
                    squares = squares + x * x
                    products = products + x * scaled[:, cols][None]
                parts[0, rows, :] = squares.reshape(BLOCK, LANES)
                parts[1, rows, :] = products.reshape(BLOCK, LANES)
            done = (c + 1) * chunk
            if done % LANES == 0 or done == length:
                rows = pl.ds(start, done - start)
                squares_rows.append(lane_sums(parts[0, rows, :]))
                products_rows.append(lane_sums(parts[1, rows, :]))
                start = done
        return jnp.concatenate(squares_rows, axis=1), jnp.concatenate(products_rows, axis=1)

    for k in range(1, tensor_count):
        for r in range(own_rows):
            squares, products = row_sums((k - 1) * own_rows + r)
            part_send[k - 1, 2 * r : 2 * r + 1, :] = squares[0:1, :]
            part_send[k - 1, 2 * r + 1 : 2 * r + 2, :] = products[0:1, :]

    pl.semaphore_wait(barrier, devices - 1)

    part_copies = []
    for k in range(1, tensor_count):
        copy = pltpu.make_async_remote_copy(
            src_ref=part_send.at[k - 1],
            dst_ref=part_recv.at[k - 1],
            send_sem=part_send_sem.at[k - 1],
            recv_sem=part_recv_sem.at[k - 1],
            device_id=(me_seq, lax.rem(me_ten + k, tensor_count)),
            device_id_type=pl.DeviceIdType.MESH,
        )
        copy.start()
        part_copies.append(copy)

    def send_all(buffer, send_sem, recv_sem):
        def send(k, _):
            pltpu.make_async_remote_copy(
                src_ref=buffer.at[my_slot],
                dst_ref=buffer.at[my_slot],
                send_sem=send_sem,
                recv_sem=recv_sem,
                device_id=peer(k),
                device_id_type=pl.DeviceIdType.MESH,
            ).start()
            return 0

        each_peer(send)

    def all_blocks(buffer, sem):
        view = buffer.at[pl.ds(0, devices - 1)]
        return pltpu.make_async_copy(view, view, sem)

    send_all(early, early_send_sem, early_recv_sem)

    own = [row_sums((tensor_count - 1) * own_rows + r) for r in range(own_rows)]
    for copy in part_copies:
        copy.wait()

    for r in range(own_rows):
        info = rows_info[r]
        trace, levels, reward, following = (
            info[name] for name in ("trace", "levels", "reward", "following")
        )
        squares, products = own[r]
        for k in range(1, tensor_count):
            squares = squares + part_recv[k - 1, 2 * r : 2 * r + 1, :]
            products = products + part_recv[k - 1, 2 * r + 1 : 2 * r + 2, :]
        values = products * lax.rsqrt(squares / width + EPS_NORM)
        values_ref[r : r + 1, :] = values[0:1, :]
        adv = reward + following * ahead(values, 1) - values
        for n in range(0, len(levels), 3):
            adv = adv + sum(level * ahead(adv, d) for d, level in levels[n : n + 3] if d < length)
        late[my_slot, r : r + 1, 0:length] = adv[0:1, :]
        late[my_slot, r : r + 1, length : length + LANES] = jnp.broadcast_to(
            values[0:1, 0:1] + trace[0:1, 0:1] * adv[0:1, 0:1], (1, LANES)
        )

    send_all(late, late_send_sem, late_recv_sem)

    all_blocks(early, early_recv_sem).wait()
    count = jnp.zeros((seq_count, length), jnp.float32)
    for t in range(tensor_count):
        for r in range(own_rows):
            count = count + early[pl.ds(t * seq_count, seq_count), r, length : 2 * length]
    total = lambda x: jnp.sum(jnp.sum(x, axis=0, keepdims=True), axis=1, keepdims=True)
    count = total(count)
    coefs = []
    for t in range(tensor_count):
        for r in range(own_rows):
            row = t * own_rows + r
            slots = pl.ds(t * seq_count, seq_count)
            coef = coef_of(early[slots, r, 2 * length : 2 * length + LANES], row)
            coefs.append(coef)
            slope[slots, r, :] = jnp.broadcast_to(trc[row] * coef[:, 0:1], (seq_count, LANES))
    all_blocks(late, late_recv_sem).wait()

    advs = []
    for t in range(tensor_count):
        for r in range(own_rows):
            entering = jnp.full((1, LANES), boot[t * own_rows + r], jnp.float32)
            for n in range(seq_count - 1, -1, -1):
                slot = t * seq_count + n
                carry[slot, r : r + 1, :] = entering
                if n:
                    offset = late[slot, r : r + 1, length : length + LANES]
                    entering = offset + slope[slot, r : r + 1, :] * entering
    sums = jnp.zeros((seq_count, length), jnp.float32)
    for t in range(tensor_count):
        for r in range(own_rows):
            slots = pl.ds(t * seq_count, seq_count)
            entering = jnp.concatenate([carry[slots, r, :]] * (length // LANES), axis=1)
            adv = late[slots, r, 0:length] + coefs[t * own_rows + r] * entering
            advs.append(adv)
            sums = sums + early[slots, r, length : 2 * length] * adv
    mean = total(sums) / count
    sums = jnp.zeros((seq_count, length), jnp.float32)
    for t in range(tensor_count):
        for r in range(own_rows):
            slots = pl.ds(t * seq_count, seq_count)
            centred = advs[t * own_rows + r] - mean
            advs[t * own_rows + r] = centred
            sums = sums + early[slots, r, length : 2 * length] * centred * centred
    scale = lax.rsqrt(total(sums) / count + EPS_WHITE)

    def token_loss(ratio, weight, white):
        clipped = jnp.clip(ratio, 1.0 - CLIP, 1.0 + CLIP)
        return -weight * jnp.minimum(ratio * white, clipped * white)

    for r in range(own_rows):
        ratio, weight = rows_info[r]["ratio"], rows_info[r]["weight"]
        coef = coef_of(early[my_slot, r : r + 1, 2 * length : 2 * length + LANES], first_row + r)
        entering = carry[my_slot, r : r + 1, :]
        entering = jnp.concatenate([entering] * (length // LANES), axis=1)
        adv = late[my_slot, r : r + 1, 0:length] + coef * entering
        white = (adv - mean) * scale
        white_ref[r : r + 1, :] = white
        token_ref[r : r + 1, :] = token_loss(ratio, weight, white)

    sums = jnp.zeros((seq_count, length), jnp.float32)
    for t in range(tensor_count):
        for r in range(own_rows):
            slots = pl.ds(t * seq_count, seq_count)
            sums = sums + token_loss(
                early[slots, r, 0:length],
                early[slots, r, length : 2 * length],
                advs[t * own_rows + r] * scale,
            )
    loss_ref[...] = jnp.broadcast_to(total(sums) / count, (1, LANES))

    all_blocks(early, early_send_sem).wait()
    all_blocks(late, late_send_sem).wait()


def write_out(*refs):
    half = len(refs) // 2
    for src, dst in zip(refs[:half], refs[half:]):
        dst[...] = src[:, : dst.shape[1]]


def shards(seq_count, tensor_count, *args):
    seqs_all, length, local_width = args[0].shape
    own_rows = seqs_all // tensor_count
    devices = seq_count * tensor_count
    chunk = min(length, 64)
    f32 = jnp.float32
    row = jax.ShapeDtypeStruct((own_rows, length), f32)
    dma = pltpu.SemaphoreType.DMA
    shapes = [row, row, row, jax.ShapeDtypeStruct((1, 1), f32)]
    outs = pl.pallas_call(
        functools.partial(kernel, seq_count, tensor_count, local_width * tensor_count, chunk),
        out_shape=[row, row, row, jax.ShapeDtypeStruct((1, LANES), f32)],
        in_specs=[pl.BlockSpec(memory_space=pltpu.HBM)] * 11,
        out_specs=[pl.BlockSpec(memory_space=pltpu.VMEM)] * 4,
        scratch_shapes=[
            pltpu.VMEM((seqs_all, length, local_width), jnp.bfloat16),
            pltpu.VMEM((local_width,), jnp.bfloat16),
            pltpu.VMEM((local_width,), jnp.bfloat16),
            pltpu.VMEM((seqs_all, length), f32),
            pltpu.VMEM((seqs_all, length), jnp.int32),
            pltpu.VMEM((own_rows, length), jnp.int32),
            pltpu.VMEM((own_rows, length), f32),
            pltpu.VMEM((own_rows, length), f32),
            pltpu.SMEM((seqs_all,), f32),
            pltpu.SMEM((seqs_all,), f32),
            pltpu.SMEM((seqs_all,), f32),
            pltpu.VMEM((8, local_width), f32),
            pltpu.VMEM((2, length, LANES), f32),
            pltpu.VMEM((max(tensor_count - 1, 1), 2 * own_rows, length), f32),
            pltpu.VMEM((max(tensor_count - 1, 1), 2 * own_rows, length), f32),
            pltpu.VMEM((devices, own_rows, 2 * length + LANES), f32),
            pltpu.VMEM((devices, own_rows, length + LANES), f32),
            pltpu.VMEM((devices, own_rows, LANES), f32),
            pltpu.VMEM((devices, own_rows, LANES), f32),
            dma((seqs_all * (length // chunk),)),
            dma((10,)),
            dma((max(tensor_count - 1, 1),)),
            dma((max(tensor_count - 1, 1),)),
            dma,
            dma,
            dma,
            dma,
        ],
        compiler_params=pltpu.CompilerParams(
            collective_id=0, has_side_effects=True, vmem_limit_bytes=24 << 20
        ),
    )(*[pltpu.with_memory_space_constraint(x, pltpu.HBM) for x in args])
    outs = pl.pallas_call(
        write_out,
        out_shape=shapes,
        in_specs=[pl.BlockSpec(memory_space=pltpu.VMEM)] * 4,
        out_specs=[pl.BlockSpec(memory_space=pltpu.VMEM)] * 4,
        compiler_params=pltpu.CompilerParams(vmem_limit_bytes=1 << 20),
    )(*outs)
    return (outs[0], outs[1], outs[2], outs[3].reshape(()))


def solution(mesh):
    in_specs = (
        P(None, "seq", "tensor"),
        P("tensor"),
        P("tensor"),
        P(None, "seq"),
        P(None, "seq"),
        P("tensor", "seq"),
        P("tensor", "seq"),
        P("tensor", "seq"),
        P(),
        P(),
        P(),
    )
    out_specs = (P("tensor", "seq"), P("tensor", "seq"), P("tensor", "seq"), P())
    body = functools.partial(shards, mesh.shape["seq"], mesh.shape["tensor"])
    return jax.shard_map(body, mesh=mesh, in_specs=in_specs, out_specs=out_specs, check_vma=False)
```
